128 devices in a mesh: dp: 16 (over z, x), mp: 8 (over y, core).
Axes of the slice: x: 4, y: 4, z: 4, core: 2. Of those that a mesh axis runs over, the one named last changes fastest.
Arguments:
- gradients: bfloat16 [8, 3584, 14336], P(None, 'dp', 'mp'), may hold values from -60 to 60
- column_slot: int32 [8, 16], replicated, may hold values from 0 to 15, as said below
- left_roots: bfloat16 [16, 8, 4, 896, 896], P('dp', 'mp'), may hold values from -1 to 5
- right_roots: bfloat16 [16, 8, 4, 896, 896], P('dp', 'mp'), may hold values from -1 to 5
Outputs:
- update: bfloat16 [8, 3584, 14336], P(None, 'dp', 'mp')
- clip_scale: float32 [], replicated
The draws below stay inside these ranges and needn't reach their ends.
Inputs may be any that keep to these rules, and one draw needn't show every extreme that they name: `column_slot`: block column c belongs to group c // 2; over all matrices, the entries of one group's block columns are a permutation of 0 to 15.
All inputs are finite; a program needn't handle non-finite values.
Results may differ from the reference program's by a relative error of at most 0.0049.
Values may be sent and summed in bfloat16 or wider, within the bound.
A program may use at most 128 MiB of HBM per device.

```python
import math
import jax
import jax.numpy as jnp
from jax import lax

D = 3584
FF = 14336
BLOCK = 896
MATRICES = 8
ROW_BLOCKS = 4
COLUMNS = 16
COLS_MP = 2
SLOTS = 16
N_MP = 8


def draw_gradients(key, part):
    keys = jax.random.split(jax.random.fold_in(key, 5), 3)
    ramp = jnp.sqrt(1.0 + 2.0 * jnp.arange(D, dtype=jnp.float32) / (D - 1)).reshape(1, D, 1)
    col_scale = jnp.exp(jax.random.uniform(keys[1], (MATRICES, 1, FF), jnp.float32, 0.0, math.log(10.0)))
    row_scale = jnp.exp(jax.random.uniform(keys[0], (MATRICES, D, 1), jnp.float32, 0.0, math.log(10.0)))
    base = jnp.clip(jax.random.normal(keys[2], (MATRICES, D, FF), jnp.float32), -6.0, 6.0)
    values = base * row_scale * col_scale * ramp / 21.5
    return jnp.clip(values, -60.0, 60.0).astype(jnp.bfloat16)


def draw_column_slot(key, part):
    keys = jax.random.split(jax.random.fold_in(key, 11), N_MP)

    def permute_one(sub_key):
        return jax.random.permutation(sub_key, SLOTS)
    perms = jax.vmap(permute_one)(keys).astype(jnp.int32)
    table = perms.reshape(N_MP, MATRICES, COLS_MP).transpose(1, 0, 2).reshape(MATRICES, COLUMNS)
    return table.astype(jnp.int32)


def draw_roots(key):
    keys = jax.random.split(key, 2)
    shape = (SLOTS, N_MP, ROW_BLOCKS, BLOCK, BLOCK)
    noise = jnp.clip(jax.random.normal(keys[0], shape, jnp.float32), -4.0, 4.0)
    symmetric = (noise + jnp.swapaxes(noise, -1, -2)) * (0.35 / math.sqrt(2.0 * BLOCK))
    diagonal = jnp.exp(jax.random.uniform(keys[1], shape[:-1], jnp.float32, math.log(0.5), math.log(2.0)))
    matrix = symmetric + diagonal[..., None] * jnp.eye(BLOCK, dtype=jnp.float32)
    return matrix.astype(jnp.bfloat16)


def draw_left_roots(key, part):
    return draw_roots(jax.random.fold_in(key, 21))


def draw_right_roots(key, part):
    return draw_roots(jax.random.fold_in(key, 37))


def setup_inputs(seed: int = 0) -> dict:
    splits = jax.random.split(jax.random.key(seed), 5)
    gradients = draw_gradients(jax.random.fold_in(splits[4], 71), 0)
    column_slot = draw_column_slot(jax.random.fold_in(splits[4], 71), 0)
    left_roots = draw_left_roots(jax.random.fold_in(splits[4], 71), 0)
    right_roots = draw_right_roots(jax.random.fold_in(splits[4], 71), 0)
    return {"gradients": gradients, "column_slot": column_slot, "left_roots": left_roots, "right_roots": right_roots}


rms_limit = 0.25
epsilon = 1e-06

def reference(gradients, column_slot, left_roots, right_roots):
    widened = gradients.astype(jnp.float32)
    square_sum = jnp.sum(widened * widened)
    mean_square = square_sum / (MATRICES * D * FF)
    clip_scale = jnp.minimum(jnp.float32(1.0), rms_limit / jnp.sqrt(mean_square + epsilon)).astype(jnp.float32)
    zero_index = jnp.zeros((), jnp.int32)

    def one_column(flat_index):
        matrix = (flat_index // COLUMNS).astype(jnp.int32)
        block_col = (flat_index % COLUMNS).astype(jnp.int32)
        group_index = (block_col // COLS_MP).astype(jnp.int32)
        slot_index = column_slot[matrix, block_col].astype(jnp.int32)
        block_grad = lax.dynamic_slice(gradients, (matrix, zero_index, (block_col * BLOCK).astype(jnp.int32)), (1, D, BLOCK))
        block_grad = block_grad.reshape(ROW_BLOCKS, BLOCK, BLOCK).astype(jnp.float32)
        starts = (slot_index, group_index, zero_index, zero_index, zero_index)
        left_root = lax.dynamic_slice(left_roots, starts, (1, 1, ROW_BLOCKS, BLOCK, BLOCK)).reshape(ROW_BLOCKS, BLOCK, BLOCK)
        right_root = lax.dynamic_slice(right_roots, starts, (1, 1, ROW_BLOCKS, BLOCK, BLOCK)).reshape(ROW_BLOCKS, BLOCK, BLOCK)
        first_product = jnp.einsum('nab,nbc->nac', left_root.astype(jnp.float32), block_grad)
        scaled = (clip_scale * first_product).astype(jnp.bfloat16)
        second_product = jnp.einsum('nab,nbc->nac', scaled.astype(jnp.float32), right_root.astype(jnp.float32))
        return second_product.astype(jnp.bfloat16).reshape(D, BLOCK)
    columns = lax.map(one_column, jnp.arange(MATRICES * COLUMNS, dtype=jnp.int32))
    update = columns.reshape(MATRICES, COLUMNS, D, BLOCK).transpose(0, 2, 1, 3).reshape(MATRICES, D, FF)
    return (update, clip_scale)
```

```python
import functools

import jax
import jax.numpy as jnp
from jax import lax
from jax.experimental import pallas as pl
from jax.experimental.pallas import tpu as pltpu
from jax.sharding import PartitionSpec as P

D = 3584
FF = 14336
BLOCK = 896
MATRICES = 8
ROW_BLOCKS = 4
ROWS = 224
N_DP = 16
N_MP = 8
COLS = 2
SLOTS = 16
PART = 32
PARTS = ROWS // PART
LIMIT = 0.25
EPSILON = 1e-6
MESH = pl.DeviceIdType.MESH


def offset(dz, dx):
    return (dz % 4) * 4 + dx % 4


NEAR = [offset(*o) for o in ((1, 0), (3, 0), (1, 1), (3, 3), (1, 3), (3, 1), (1, 2), (3, 2))]
REST = [offset(*o) for o in ((0, 1), (0, 3), (2, 0), (2, 1), (2, 3), (0, 2), (2, 2))]


def exchange_kernel(
    slot, gradients, left, right, ret, clip_out,
    own, send, recv, lbuf, rbuf, inverse, acc, mp_sums, dp_sums,
    own_sem, root_sem, fwd_send, fwd_recv, ret_send, ret_recv, mp_send, mp_recv, dp_send, dp_recv,
):
    me = lax.axis_index("dp")
    mp = lax.axis_index("mp")
    z, x = me // 4, me % 4

    def device(k):
        return lax.rem(z + k // 4, 4) * 4 + lax.rem(x + k % 4, 4)

    loads = []
    for c in range(COLS):
        for m in range(MATRICES):
            copy = pltpu.make_async_copy(
                gradients.at[m, :, pl.ds(c * BLOCK, BLOCK)], own.at[c * MATRICES + m], own_sem.at[c * MATRICES + m]
            )
            copy.start()
            loads.append(copy)

    barrier = pltpu.get_barrier_semaphore()
    for k in range(1, N_DP):
        pl.semaphore_signal(barrier, inc=1, device_id={"dp": device(k)}, device_id_type=MESH)
    for k in range(1, N_MP):
        pl.semaphore_signal(barrier, inc=1, device_id={"mp": lax.rem(mp + k, N_MP)}, device_id_type=MESH)

    slots = [slot[m, mp * COLS + c] for c in range(COLS) for m in range(MATRICES)]
    for k in range(N_DP):
        target = device(k)
        found = jnp.int32(0)
        for j, value in enumerate(slots):
            found = jnp.where(value == target, jnp.int32(j), found)
        inverse[k] = found

    for copy in loads:
        copy.wait()
    roots = []
    for r in range(ROW_BLOCKS):
        for h, (src, dst) in enumerate(((left, lbuf), (right, rbuf))):
            copy = pltpu.make_async_copy(src.at[0, 0, r], dst.at[r], root_sem.at[2 * r + h])
            copy.start()
            roots.append(copy)

    acc[...] = jnp.zeros_like(acc)

    def stage(p):
        rows = pl.ds(p * PART, PART)
        total = acc[...]
        for k in range(N_DP):
            block = own[inverse[k], rows, :]
            if k == 0:
                recv[z, pl.ds(x * ROWS + p * PART, PART), :] = block
            else:
                send[k, rows, :] = block
            wide = block.astype(jnp.float32)
            square = wide * wide
            for lane in range(0, BLOCK, 128):
                total = total + square[:, lane : lane + 128]
        acc[...] = total

    def send_part(k, p):
        rows = pl.ds(p * PART, PART)
        pltpu.make_async_remote_copy(
            src_ref=send.at[k, rows],
            dst_ref=recv.at[z, pl.ds(x * ROWS + p * PART, PART)],
            send_sem=fwd_send.at[k],
            recv_sem=fwd_recv.at[k // 4],
            device_id={"dp": device(k)},
            device_id_type=MESH,
        ).start()

    def send_parts(offsets, first, last):
        @pl.loop(first, last)
        def _(p):
            for k in offsets:
                send_part(k, p)

    stage(0)
    stage(1)
    pl.semaphore_wait(barrier, N_DP + N_MP - 2)
    send_parts(NEAR, 0, 1)

    @pl.loop(2, PARTS)
    def _(p):
        stage(p)

    send_parts(NEAR, 1, 2)

    part = acc[...]
    mp_sums[mp] = part[0:8] + part[8:16] + part[16:24] + part[24:32]
    mp_copies = []
    for k in range(1, N_MP):
        copy = pltpu.make_async_remote_copy(
            src_ref=mp_sums.at[mp],
            dst_ref=mp_sums.at[mp],
            send_sem=mp_send.at[k],
            recv_sem=mp_recv.at[k],
            device_id={"mp": lax.rem(mp + k, N_MP)},
            device_id_type=MESH,
        )
        copy.start()
        mp_copies.append(copy)
    for copy in mp_copies:
        copy.wait()
    total = mp_sums[0]
    for i in range(1, N_MP):
        total = total + mp_sums[i]
    dp_sums[me] = total
    dp_copies = []
    for k in range(1, N_DP):
        copy = pltpu.make_async_remote_copy(
            src_ref=dp_sums.at[me],
            dst_ref=dp_sums.at[me],
            send_sem=dp_send.at[k],
            recv_sem=dp_recv.at[k],
            device_id={"dp": device(k)},
            device_id_type=MESH,
        )
        copy.start()
        dp_copies.append(copy)

    send_parts(NEAR, 2, PARTS)
    send_parts(REST, 0, PARTS)

    for copy in dp_copies:
        copy.wait()
    total = dp_sums[0]
    for i in range(1, N_DP):
        total = total + dp_sums[i]
    square_sum = jnp.broadcast_to(jnp.sum(total, keepdims=True), (8, 128))
    clip = jnp.minimum(jnp.float32(1.0), LIMIT / jnp.sqrt(square_sum / (MATRICES * D * FF) + EPSILON))
    clip_out[...] = clip
    scale = jnp.broadcast_to(clip[0:1, 0:1], (1, BLOCK))

    for copy in roots:
        copy.wait()

    def wait_block(dz):
        rows = BLOCK if dz else BLOCK - ROWS
        pltpu.make_async_copy(
            recv.at[0, pl.ds(0, rows)], recv.at[0, pl.ds(0, rows)], fwd_recv.at[dz]
        ).wait()

    def compute(dz):
        wait_block(dz)
        r = lax.rem(z + 4 - dz, 4)

        @pl.loop(0, 4)
        def _(i):
            product = jnp.dot(lbuf[r, pl.ds(i * ROWS, ROWS), :], recv[r], preferred_element_type=jnp.float32)
            scaled = (scale * product).astype(jnp.bfloat16)
            second = jnp.dot(scaled, rbuf[r], preferred_element_type=jnp.float32)
            own[r * 4 + i] = second.astype(jnp.bfloat16)

    def return_part(k, p):
        rows = pl.ds(p * PART, PART)
        pltpu.make_async_remote_copy(
            src_ref=own.at[device(k), rows],
            dst_ref=ret.at[me, rows],
            send_sem=ret_send.at[k],
            recv_sem=ret_recv.at[k],
            device_id={"dp": device(k)},
            device_id_type=MESH,
        ).start()

    def return_parts(offsets):
        @pl.loop(0, PARTS)
        def _(p):
            for k in offsets:
                return_part(k, p)

    compute(1)
    compute(3)
    return_parts(NEAR)
    compute(2)
    compute(0)
    return_parts(REST)
    ret[me] = own[me]

    for k in range(1, N_DP):
        for sem in (fwd_send, ret_send, ret_recv):
            pltpu.make_async_copy(send.at[k], send.at[k], sem.at[k]).wait()


def place_kernel(slot, ret, update, sem):
    mp = lax.axis_index("mp")
    copies = []
    for c in range(COLS):
        for m in range(MATRICES):
            copy = pltpu.make_async_copy(
                ret.at[slot[m, mp * COLS + c]], update.at[m, :, pl.ds(c * BLOCK, BLOCK)], sem.at[c * MATRICES + m]
            )
            copy.start()
            copies.append(copy)
    for copy in copies:
        copy.wait()


def body(gradients, column_slot, left_roots, right_roots):
    block = (ROW_BLOCKS, BLOCK, BLOCK)
    columns = (SLOTS, ROWS, BLOCK)
    bf16, f32 = jnp.bfloat16, jnp.float32
    dma = pltpu.SemaphoreType.DMA
    anywhere = pl.BlockSpec(memory_space=pl.ANY)
    vmem = pl.BlockSpec(memory_space=pltpu.VMEM)
    smem = pl.BlockSpec(memory_space=pltpu.SMEM)
    ret, clip = pl.pallas_call(
        exchange_kernel,
        out_shape=(jax.ShapeDtypeStruct(columns, bf16), jax.ShapeDtypeStruct((8, 128), f32)),
        in_specs=[smem, anywhere, anywhere, anywhere],
        out_specs=(vmem, vmem),
        scratch_shapes=[
            pltpu.VMEM(columns, bf16),
            pltpu.VMEM(columns, bf16),
            pltpu.VMEM(block, bf16),
            pltpu.VMEM(block, bf16),
            pltpu.VMEM(block, bf16),
            pltpu.SMEM((N_DP,), jnp.int32),
            pltpu.VMEM((PART, 128), f32),
            pltpu.VMEM((N_MP, 8, 128), f32),
            pltpu.VMEM((N_DP, 8, 128), f32),
            dma((COLS * MATRICES,)),
            dma((2 * ROW_BLOCKS,)),
            dma((N_DP,)),
            dma((4,)),
            dma((N_DP,)),
            dma((N_DP,)),
            dma((N_MP,)),
            dma((N_MP,)),
            dma((N_DP,)),
            dma((N_DP,)),
        ],
        compiler_params=pltpu.CompilerParams(
            collective_id=0, has_side_effects=True, vmem_limit_bytes=54 * 2**20
        ),
        name="exchange",
    )(column_slot, gradients, left_roots, right_roots)
    update = pl.pallas_call(
        place_kernel,
        out_shape=jax.ShapeDtypeStruct((MATRICES, ROWS, COLS * BLOCK), bf16),
        in_specs=[smem, vmem],
        out_specs=anywhere,
        scratch_shapes=[dma((COLS * MATRICES,))],
        compiler_params=pltpu.CompilerParams(vmem_limit_bytes=12 * 2**20),
        name="place",
    )(column_slot, ret)
    return update, clip[0, 0]


def solution(mesh):
    return jax.shard_map(
        body,
        mesh=mesh,
        in_specs=(P(None, "dp", "mp"), P(), P("dp", "mp"), P("dp", "mp")),
        out_specs=(P(None, "dp", "mp"), P()),
        check_vma=False,
    )
```

```python
import functools

import jax
import jax.numpy as jnp
from jax import lax
from jax.experimental import pallas as pl
from jax.experimental.pallas import tpu as pltpu
from jax.sharding import PartitionSpec as P

D = 3584
FF = 14336
BLOCK = 896
MATRICES = 8
ROW_BLOCKS = 4
ROWS = 224
N_DP = 16
N_MP = 8
COLS = 2
SLOTS = 16
PART = 56
PARTS = ROWS // PART
SENT_WINDOW = 4
LEAD = 0
DEPUTY = 1
ORDER = "RRNRNRNN" + "RRRNRNNN"
PLAN = "1 2 3 L 4 5 6 7 T C D 8 9 10 A B 11 12 13 14 15"
LIMIT = 0.25
EPSILON = 1e-6
MESH = pl.DeviceIdType.MESH


def offset(dz, dx):
    return (dz % 4) * 4 + dx % 4


NEAR = [offset(*o) for o in ((1, 0), (3, 0), (1, 1), (3, 3), (1, 3), (3, 1), (1, 2), (3, 2))]
REST = [offset(*o) for o in ((0, 1), (0, 3), (2, 0), (2, 1), (2, 3), (0, 2), (2, 2))]


def exchange_kernel(
    slot_table, gradients, left, right, ret, clip_out,
    slot, first, own, send, recv, lbuf, rbuf, inverse, acc, dp_sums, mp_sums, total_sum,
    entered, slot_sem, first_sem, own_sem, root_sem, sent_sem, came_sem, sum_send, sum_recv,
):
    me = lax.axis_index("dp")
    mp = lax.axis_index("mp")
    z, x = me // 4, me % 4
    leads = me == LEAD

    def device(k):
        return lax.rem(z + k // 4, 4) * 4 + lax.rem(x + k % 4, 4)

    slot_copy = pltpu.make_async_copy(slot_table, slot, slot_sem)
    slot_copy.start()

    barrier = pltpu.get_barrier_semaphore()
    for k in range(1, N_DP):
        target = device(k)

        @pl.when(target != LEAD)
        def _(target=target):
            pl.semaphore_signal(barrier, inc=1, device_id={"dp": target}, device_id_type=MESH)

    @pl.when(leads)
    def _():
        for k in range(1, N_MP):
            pl.semaphore_signal(barrier, inc=1, device_id={"mp": lax.rem(mp + k, N_MP)}, device_id_type=MESH)

    def load(row, rows, dst, sems):
        copies = []
        for c in range(COLS):
            for m in range(MATRICES):
                j = c * MATRICES + m
                copy = pltpu.make_async_copy(
                    gradients.at[m, pl.ds(row, rows), pl.ds(c * BLOCK, BLOCK)],
                    dst.at[j, pl.ds(row, rows)],
                    sems.at[j],
                )
                copy.start()
                copies.append(copy)
        return copies

    first_loads = load(0, PART, first, first_sem)
    loads = load(PART, ROWS - PART, own, own_sem)
    slot_copy.wait()

    slots = [slot[m, mp * COLS + c] for c in range(COLS) for m in range(MATRICES)]
    for k in range(N_DP):
        target = device(k)
        found = jnp.int32(0)
        for j, value in enumerate(slots):
            found = jnp.where(value == target, jnp.int32(j), found)
        inverse[k] = found

    for copy in first_loads:
        copy.wait()

    acc[...] = jnp.zeros_like(acc)

    def stage(p, source):
        rows = pl.ds(p * PART, PART)
        total = acc[...]
        for k in range(N_DP):
            block = source[inverse[k], rows, :]
            if k == 0:
                recv[z, pl.ds(x * ROWS + p * PART, PART), :] = block
            else:
                send[k, rows, :] = block
            wide = block.astype(jnp.float32)
            square = wide * wide
            for lane in range(0, BLOCK, 128):
                total = total + square[:, lane : lane + 128]
        acc[...] = total

    def wait_rows(rows, sem):
        view = recv.at[0, pl.ds(0, rows)]
        pltpu.make_async_copy(view, view, sem).wait()

    def group(g):
        start = g - g % (2 * PARTS)
        return NEAR if ORDER[g] == "N" else REST, ORDER[start:g].count(ORDER[g])

    waited = {"sent": set(), "came": set()}

    def wait(kind, groups):
        sems = sent_sem if kind == "sent" else came_sem
        for g in groups:
            if g not in waited[kind]:
                wait_rows(len(group(g)[0]) * PART, sems.at[g])
                waited[kind].add(g)

    def issue(g):
        wait("sent", range(g + 1 - SENT_WINDOW))
        offsets, p = group(g)
        rows = pl.ds(p * PART, PART)
        for k in offsets:
            target = device(k)
            if g < 2 * PARTS:
                src, dst = send.at[k, rows], recv.at[z, pl.ds(x * ROWS + p * PART, PART)]
            else:
                src, dst = own.at[target, rows], ret.at[me, rows]
            pltpu.make_async_remote_copy(
                src_ref=src, dst_ref=dst, send_sem=sent_sem.at[g], recv_sem=came_sem.at[g],
                device_id={"dp": target}, device_id_type=MESH,
            ).start()

    stage(0, first)

    @pl.when(jnp.logical_not(leads))
    def _():
        pl.semaphore_wait(barrier, N_DP - 1)

    @pl.when(me == DEPUTY)
    def _():
        pl.semaphore_signal(entered, inc=1, device_id={"dp": LEAD}, device_id_type=MESH)

    @pl.when(leads)
    def _():
        pl.semaphore_wait(entered, 1)

    issue(0)
    for copy in loads:
        copy.wait()
    roots = []
    for r in range(ROW_BLOCKS):
        for h, (src, dst) in enumerate(((left, lbuf), (right, rbuf))):
            copy = pltpu.make_async_copy(src.at[0, 0, r], dst.at[r], root_sem.at[2 * r + h])
            copy.start()
            roots.append(copy)

    @pl.loop(1, PARTS)
    def _(p):
        stage(p, own)

    part = acc[...]
    dp_sums[me] = sum((part[i : i + 8] for i in range(8, PART, 8)), part[0:8])

    def to_lead():
        return pltpu.make_async_remote_copy(
            src_ref=dp_sums.at[me], dst_ref=dp_sums.at[me], send_sem=sum_send.at[0], recv_sem=sum_recv.at[0],
            device_id={"dp": LEAD}, device_id_type=MESH,
        )

    @pl.when(jnp.logical_not(leads))
    def _():
        to_lead().start()

    def wait_sums(ref, count, sem):
        view = ref.at[pl.ds(0, count)]
        pltpu.make_async_copy(view, view, sem).wait()

    def lead_sums():
        wait_sums(dp_sums, N_DP - 1, sum_recv.at[0])
        total = dp_sums[0]
        for i in range(1, N_DP):
            total = total + dp_sums[i]
        mp_sums[mp] = total
        pl.semaphore_wait(barrier, N_MP - 1)
        for k in range(1, N_MP):
            pltpu.make_async_remote_copy(
                src_ref=mp_sums.at[mp], dst_ref=mp_sums.at[mp], send_sem=sum_send.at[1], recv_sem=sum_recv.at[1],
                device_id={"mp": lax.rem(mp + k, N_MP)}, device_id_type=MESH,
            ).start()
        wait_sums(mp_sums, N_MP - 1, sum_send.at[1])
        wait_sums(mp_sums, N_MP - 1, sum_recv.at[1])
        total = mp_sums[0]
        for i in range(1, N_MP):
            total = total + mp_sums[i]
        total_sum[...] = total
        for k in range(1, N_DP):
            pltpu.make_async_remote_copy(
                src_ref=total_sum, dst_ref=total_sum, send_sem=sum_send.at[2], recv_sem=sum_recv.at[2],
                device_id={"dp": device(k)}, device_id_type=MESH,
            ).start()

    def finish_sums():
        @pl.when(jnp.logical_not(leads))
        def _():
            to_lead().wait_send()
            pltpu.make_async_copy(total_sum, total_sum, sum_recv.at[2]).wait()

        square_sum = jnp.broadcast_to(jnp.sum(total_sum[...], keepdims=True), (8, 128))
        clip = jnp.minimum(jnp.float32(1.0), LIMIT / jnp.sqrt(square_sum / (MATRICES * D * FF) + EPSILON))
        clip_out[...] = clip
        for copy in roots:
            copy.wait()

    def compute(dz):
        wait("came", [g for g in range(2 * PARTS) if ORDER[g] == ("N" if dz % 2 else "R")])
        r = lax.rem(z + 4 - dz, 4)
        scale = jnp.broadcast_to(clip_out[0:1, 0:1], (1, BLOCK))

        @pl.loop(0, 4)
        def _(i):
            product = jnp.dot(lbuf[r, pl.ds(i * ROWS, ROWS), :], recv[r], preferred_element_type=jnp.float32)
            scaled = (scale * product).astype(jnp.bfloat16)
            second = jnp.dot(scaled, rbuf[r], preferred_element_type=jnp.float32)
            own[r * 4 + i] = second.astype(jnp.bfloat16)

    for step in PLAN.split():
        if step.isdigit():
            issue(int(step))
        elif step == "L":
            pl.when(leads)(lead_sums)
        elif step == "T":
            finish_sums()
        else:
            compute({"A": 1, "B": 3, "C": 2, "D": 0}[step])
    ret[me] = own[me]
    wait("sent", range(4 * PARTS))
    wait("came", range(4 * PARTS))

    @pl.when(leads)
    def _():
        wait_sums(dp_sums, N_DP - 1, sum_send.at[2])


def place_kernel(slot, ret, clip, update, clip_out, clip_one, clip_sem, sem):
    mp = lax.axis_index("mp")
    clip_one[...] = clip[0:1, 0:1]
    clip_copy = pltpu.make_async_copy(clip_one, clip_out, clip_sem)
    clip_copy.start()
    copies = []
    for c in range(COLS):
        for m in range(MATRICES):
            copy = pltpu.make_async_copy(
                ret.at[slot[m, mp * COLS + c]], update.at[m, :, pl.ds(c * BLOCK, BLOCK)], sem.at[c * MATRICES + m]
            )
            copy.start()
            copies.append(copy)
    for copy in copies:
        copy.wait()
    clip_copy.wait()


def body(gradients, column_slot, left_roots, right_roots):
    block = (ROW_BLOCKS, BLOCK, BLOCK)
    columns = (SLOTS, ROWS, BLOCK)
    bf16, f32 = jnp.bfloat16, jnp.float32
    dma = pltpu.SemaphoreType.DMA
    anywhere = pl.BlockSpec(memory_space=pl.ANY)
    vmem = pl.BlockSpec(memory_space=pltpu.VMEM)
    smem = pl.BlockSpec(memory_space=pltpu.SMEM)
    ret, clip = pl.pallas_call(
        exchange_kernel,
        out_shape=(pltpu.VMEM(columns, bf16), pltpu.VMEM((8, 128), f32)),
        in_specs=[anywhere, anywhere, anywhere, anywhere],
        out_specs=(vmem, vmem),
        scratch_shapes=[
            pltpu.SMEM((MATRICES, COLS * N_MP), jnp.int32),
            pltpu.VMEM((SLOTS, PART, BLOCK), bf16),
            pltpu.VMEM(columns, bf16),
            pltpu.VMEM(columns, bf16),
            pltpu.VMEM(block, bf16),
            pltpu.VMEM(block, bf16),
            pltpu.VMEM(block, bf16),
            pltpu.SMEM((N_DP,), jnp.int32),
            pltpu.VMEM((PART, 128), f32),
            pltpu.VMEM((N_DP, 8, 128), f32),
            pltpu.VMEM((N_MP, 8, 128), f32),
            pltpu.VMEM((8, 128), f32),
            pltpu.SemaphoreType.REGULAR,
            dma,
            dma((COLS * MATRICES,)),
            dma((COLS * MATRICES,)),
            dma((2 * ROW_BLOCKS,)),
            dma((4 * PARTS,)),
            dma((4 * PARTS,)),
            dma((3,)),
            dma((3,)),
        ],
        compiler_params=pltpu.CompilerParams(
            collective_id=0, has_side_effects=True, vmem_limit_bytes=54 * 2**20
        ),
        name="exchange",
    )(column_slot, gradients, left_roots, right_roots)
    update, clip = pl.pallas_call(
        place_kernel,
        out_shape=(
            jax.ShapeDtypeStruct((MATRICES, ROWS, COLS * BLOCK), bf16),
            jax.ShapeDtypeStruct((1, 1), f32),
        ),
        in_specs=[smem, vmem, vmem],
        out_specs=(anywhere, anywhere),
        scratch_shapes=[pltpu.VMEM((1, 1), f32), dma, dma((COLS * MATRICES,))],
        compiler_params=pltpu.CompilerParams(vmem_limit_bytes=8 * 2**20),
        name="place",
    )(
        column_slot,
        pltpu.with_memory_space_constraint(ret, pltpu.VMEM),
        pltpu.with_memory_space_constraint(clip, pltpu.VMEM),
    )
    return update, clip[0, 0]


def solution(mesh):
    return jax.shard_map(
        body,
        mesh=mesh,
        in_specs=(P(None, "dp", "mp"), P(), P("dp", "mp"), P("dp", "mp")),
        out_specs=(P(None, "dp", "mp"), P()),
        check_vma=False,
    )
```

```python
import functools

import jax
import jax.numpy as jnp
from jax import lax
from jax.experimental import pallas as pl
from jax.experimental.pallas import tpu as pltpu
from jax.sharding import PartitionSpec as P

D = 3584
FF = 14336
BLOCK = 896
MATRICES = 8
ROW_BLOCKS = 4
ROWS = 224
N_DP = 16
N_MP = 8
COLS = 2
SLOTS = 16
SIZES = (56, 56, 56, 56)
BACK_SIZES = (56, 56, 56, 56)
PARTS = len(SIZES)
FIRST = SIZES[0]
STEP = SIZES[1]
LANES = 56
SENT_WINDOW = 4
LEAD = 15
DEPUTY = 14
ORDER = "RRNRNRNN" + "RRRNRNNN"
PLAN = "1 2 3 L 4 5 6 7 T C D 8 9 10 A B 11 12 13 14 15"
LIMIT = 0.25
EPSILON = 1e-6
MESH = pl.DeviceIdType.MESH


def offset(dz, dx):
    return (dz % 4) * 4 + dx % 4


NEAR = [offset(*o) for o in ((1, 0), (3, 0), (1, 1), (3, 3), (1, 3), (3, 1), (1, 2), (3, 2))]
REST = [offset(*o) for o in ((0, 1), (0, 3), (2, 0), (2, 1), (2, 3), (0, 2), (2, 2))]


def exchange_kernel(
    slot_table, gradients, left, right, update, clip_out,
    slot, first, own, send, recv, lbuf, rbuf, inverse, acc, dp_sums, mp_sums, total_sum,
    ret_0, ret_1, ret_2, ret_3,
    entered, slot_sem, first_sem, own_sem, root_sem, sent_sem, came_sem, sum_send, sum_recv,
):
    me = lax.axis_index("dp")
    mp = lax.axis_index("mp")
    z, x = me // 4, me % 4
    leads = me == LEAD
    ret = (ret_0, ret_1, ret_2, ret_3)

    def device(k):
        return lax.rem(z + k // 4, 4) * 4 + lax.rem(x + k % 4, 4)

    slot_copy = pltpu.make_async_copy(slot_table, slot, slot_sem)
    slot_copy.start()

    barrier = pltpu.get_barrier_semaphore()
    for k in range(1, N_DP):
        target = device(k)

        @pl.when(target != LEAD)
        def _(target=target):
            pl.semaphore_signal(barrier, inc=1, device_id={"dp": target}, device_id_type=MESH)

    @pl.when(leads)
    def _():
        for k in range(1, N_MP):
            pl.semaphore_signal(barrier, inc=1, device_id={"mp": lax.rem(mp + k, N_MP)}, device_id_type=MESH)

    def load(row, rows, dst, sems):
        copies = []
        for c in range(COLS):
            for m in range(MATRICES):
                j = c * MATRICES + m
                copy = pltpu.make_async_copy(
                    gradients.at[m, pl.ds(row, rows), pl.ds(c * BLOCK, BLOCK)],
                    dst.at[j, pl.ds(row, rows)],
                    sems.at[j],
                )
                copy.start()
                copies.append(copy)
        return copies

    first_loads = load(0, FIRST, first, first_sem)
    slot_copy.wait()

    slots = [slot[m, mp * COLS + c] for c in range(COLS) for m in range(MATRICES)]
    for k in range(N_DP):
        target = device(k)
        found = jnp.int32(0)
        for j, value in enumerate(slots):
            found = jnp.where(value == target, jnp.int32(j), found)
        inverse[k] = found

    for copy in first_loads:
        copy.wait()
    loads = load(FIRST, ROWS - FIRST, own, own_sem)

    acc[...] = jnp.zeros_like(acc)

    def stage(start, size, source):
        rows = pl.ds(start, size)
        total = acc[...]
        for k in range(N_DP):
            block = source[inverse[k], rows, :]
            if k == 0:
                recv[z, pl.ds(x * ROWS + start, size), :] = block
            else:
                send[k, rows, :] = block
            wide = block.astype(jnp.float32)
            square = wide * wide
            for row in range(0, size, LANES):
                for lane in range(0, BLOCK, 128):
                    total = total + square[row : row + LANES, lane : lane + 128]
        acc[...] = total

    def wait_rows(rows, sem):
        view = recv.at[0, pl.ds(0, rows)]
        pltpu.make_async_copy(view, view, sem).wait()

    def group(g):
        start = g - g % (2 * PARTS)
        sizes = SIZES if g < 2 * PARTS else BACK_SIZES
        p = ORDER[start:g].count(ORDER[g])
        return NEAR if ORDER[g] == "N" else REST, sum(sizes[:p]), sizes[p], p

    waited = {"sent": set(), "came": set()}

    def wait(kind, groups):
        sems = sent_sem if kind == "sent" else came_sem
        for g in groups:
            if g not in waited[kind]:
                offsets, _, size, _ = group(g)
                wait_rows(len(offsets) * size, sems.at[g])
                waited[kind].add(g)

    def issue(g):
        wait("sent", range(g + 1 - SENT_WINDOW))
        offsets, start, size, p = group(g)
        rows = pl.ds(start, size)
        for k in offsets:
            target = device(k)
            if g < 2 * PARTS:
                src, dst = send.at[k, rows], recv.at[z, pl.ds(x * ROWS + start, size)]
            else:
                src, dst = own.at[target, rows], ret[p].at[me]
            pltpu.make_async_remote_copy(
                src_ref=src, dst_ref=dst, send_sem=sent_sem.at[g], recv_sem=came_sem.at[g],
                device_id={"dp": target}, device_id_type=MESH,
            ).start()

    stage(0, FIRST, first)

    @pl.when(jnp.logical_not(leads))
    def _():
        pl.semaphore_wait(barrier, N_DP - 1)

    @pl.when(me == DEPUTY)
    def _():
        pl.semaphore_signal(entered, inc=1, device_id={"dp": LEAD}, device_id_type=MESH)

    @pl.when(leads)
    def _():
        pl.semaphore_wait(entered, 1)

    issue(0)
    for copy in loads:
        copy.wait()
    roots = []
    for r in range(ROW_BLOCKS):
        for h, (src, dst) in enumerate(((left, lbuf), (right, rbuf))):
            copy = pltpu.make_async_copy(src.at[0, 0, r], dst.at[r], root_sem.at[2 * r + h])
            copy.start()
            roots.append(copy)

    @pl.loop(1, PARTS)
    def _(p):
        stage(FIRST + (p - 1) * STEP, STEP, own)

    part = acc[...]
    dp_sums[me] = sum((part[i : i + 8] for i in range(8, LANES, 8)), part[0:8])

    def to_lead():
        return pltpu.make_async_remote_copy(
            src_ref=dp_sums.at[me], dst_ref=dp_sums.at[me], send_sem=sum_send.at[0], recv_sem=sum_recv.at[0],
            device_id={"dp": LEAD}, device_id_type=MESH,
        )

    @pl.when(jnp.logical_not(leads))
    def _():
        to_lead().start()

    def wait_sums(ref, count, sem):
        view = ref.at[pl.ds(0, count)]
        pltpu.make_async_copy(view, view, sem).wait()

    def lead_sums():
        wait_sums(dp_sums, N_DP - 1, sum_recv.at[0])
        total = dp_sums[0]
        for i in range(1, N_DP):
            total = total + dp_sums[i]
        mp_sums[mp] = total
        pl.semaphore_wait(barrier, N_MP - 1)
        for k in range(1, N_MP):
            pltpu.make_async_remote_copy(
                src_ref=mp_sums.at[mp], dst_ref=mp_sums.at[mp], send_sem=sum_send.at[1], recv_sem=sum_recv.at[1],
                device_id={"mp": lax.rem(mp + k, N_MP)}, device_id_type=MESH,
            ).start()
        wait_sums(mp_sums, N_MP - 1, sum_send.at[1])
        wait_sums(mp_sums, N_MP - 1, sum_recv.at[1])
        total = mp_sums[0]
        for i in range(1, N_MP):
            total = total + mp_sums[i]
        total_sum[...] = total
        for k in range(1, N_DP):
            pltpu.make_async_remote_copy(
                src_ref=total_sum, dst_ref=total_sum, send_sem=sum_send.at[2], recv_sem=sum_recv.at[2],
                device_id={"dp": device(k)}, device_id_type=MESH,
            ).start()

    def finish_sums():
        @pl.when(jnp.logical_not(leads))
        def _():
            to_lead().wait_send()
            pltpu.make_async_copy(total_sum, total_sum, sum_recv.at[2]).wait()

        square_sum = jnp.broadcast_to(jnp.sum(total_sum[...], keepdims=True), (8, 128))
        clip = jnp.minimum(jnp.float32(1.0), LIMIT / jnp.sqrt(square_sum / (MATRICES * D * FF) + EPSILON))
        clip_out[...] = clip
        for copy in roots:
            copy.wait()

    def compute(dz):
        wait("came", [g for g in range(2 * PARTS) if ORDER[g] == ("N" if dz % 2 else "R")])
        r = lax.rem(z + 4 - dz, 4)
        scale = jnp.broadcast_to(clip_out[0:1, 0:1], (1, BLOCK))

        @pl.loop(0, 4)
        def _(i):
            product = jnp.dot(lbuf[r, pl.ds(i * ROWS, ROWS), :], recv[r], preferred_element_type=jnp.float32)
            scaled = (scale * product).astype(jnp.bfloat16)
            second = jnp.dot(scaled, rbuf[r], preferred_element_type=jnp.float32)
            own[r * 4 + i] = second.astype(jnp.bfloat16)

    for step in PLAN.split():
        if step.isdigit():
            issue(int(step))
        elif step == "L":
            pl.when(leads)(lead_sums)
        elif step == "T":
            finish_sums()
        else:
            compute({"A": 1, "B": 3, "C": 2, "D": 0}[step])
    for p in range(PARTS):
        start, size = sum(BACK_SIZES[:p]), BACK_SIZES[p]
        rows = pl.ds(start, size)
        ret[p][me] = own[me, rows, :]
        wait("came", [g for g in range(2 * PARTS, 4 * PARTS) if group(g)[3] == p])
        for c in range(COLS):
            for m in range(MATRICES):
                update[m, rows, pl.ds(c * BLOCK, BLOCK)] = ret[p][slot[m, mp * COLS + c]]
    wait("sent", range(4 * PARTS))

    @pl.when(leads)
    def _():
        wait_sums(dp_sums, N_DP - 1, sum_send.at[2])


def place_kernel(columns, clip, update, clip_out, clip_one, clip_sem, sem):
    clip_one[...] = clip[0:1, 0:1]
    copies = [pltpu.make_async_copy(columns.at[m], update.at[m], sem.at[m]) for m in range(MATRICES)]
    copies.append(pltpu.make_async_copy(clip_one, clip_out, clip_sem))
    for copy in copies:
        copy.start()
    for copy in copies:
        copy.wait()


def body(gradients, column_slot, left_roots, right_roots):
    block = (ROW_BLOCKS, BLOCK, BLOCK)
    columns = (SLOTS, ROWS, BLOCK)
    bf16, f32 = jnp.bfloat16, jnp.float32
    dma = pltpu.SemaphoreType.DMA
    anywhere = pl.BlockSpec(memory_space=pl.ANY)
    vmem = pl.BlockSpec(memory_space=pltpu.VMEM)
    ret, clip = pl.pallas_call(
        exchange_kernel,
        out_shape=(pltpu.VMEM((MATRICES, ROWS, COLS * BLOCK), bf16), pltpu.VMEM((8, 128), f32)),
        in_specs=[anywhere, anywhere, anywhere, anywhere],
        out_specs=(vmem, vmem),
        scratch_shapes=[
            pltpu.SMEM((MATRICES, COLS * N_MP), jnp.int32),
            pltpu.VMEM((SLOTS, FIRST, BLOCK), bf16),
            pltpu.VMEM(columns, bf16),
            pltpu.VMEM(columns, bf16),
            pltpu.VMEM(block, bf16),
            pltpu.VMEM(block, bf16),
            pltpu.VMEM(block, bf16),
            pltpu.SMEM((N_DP,), jnp.int32),
            pltpu.VMEM((LANES, 128), f32),
            pltpu.VMEM((N_DP, 8, 128), f32),
            pltpu.VMEM((N_MP, 8, 128), f32),
            pltpu.VMEM((8, 128), f32),
            *[pltpu.VMEM((SLOTS, size, BLOCK), bf16) for size in BACK_SIZES],
            pltpu.SemaphoreType.REGULAR,
            dma,
            dma((COLS * MATRICES,)),
            dma((COLS * MATRICES,)),
            dma((2 * ROW_BLOCKS,)),
            dma((4 * PARTS,)),
            dma((4 * PARTS,)),
            dma((3,)),
            dma((3,)),
        ],
        compiler_params=pltpu.CompilerParams(
            collective_id=0, has_side_effects=True, vmem_limit_bytes=54 * 2**20
        ),
        name="exchange",
    )(column_slot, gradients, left_roots, right_roots)
    update, clip = pl.pallas_call(
        place_kernel,
        out_shape=(
            jax.ShapeDtypeStruct((MATRICES, ROWS, COLS * BLOCK), bf16),
            jax.ShapeDtypeStruct((1, 1), f32),
        ),
        in_specs=[vmem, vmem],
        out_specs=(anywhere, anywhere),
        scratch_shapes=[pltpu.VMEM((1, 1), f32), dma, dma((MATRICES,))],
        compiler_params=pltpu.CompilerParams(vmem_limit_bytes=8 * 2**20),
        name="place",
    )(
        pltpu.with_memory_space_constraint(ret, pltpu.VMEM),
        pltpu.with_memory_space_constraint(clip, pltpu.VMEM),
    )
    return update, clip[0, 0]


def solution(mesh):
    return jax.shard_map(
        body,
        mesh=mesh,
        in_specs=(P(None, "dp", "mp"), P(), P("dp", "mp"), P("dp", "mp")),
        out_specs=(P(None, "dp", "mp"), P()),
        check_vma=False,
    )
```
